32 devices in a mesh: row: 4 (over y, x), col: 8 (over z, core).
Axes of the slice: x: 2, y: 2, z: 4, core: 2. Of those that a mesh axis runs over, the one named last changes fastest.
Arguments:
- right_side: bfloat16 [4, 8, 8, 128, 256], P('row', 'col'), may hold values from -6 to 6
- diag_inverse: bfloat16 [4, 8, 8, 128, 128], P('row', 'col'), may hold values from -0.5 to 0.5
- panels: bfloat16 [7, 4, 400, 128, 128], P(None, 'row', 'col'), may hold values from -0.0546875 to 0.0546875
- tile_source: int32 [7, 4, 400], P(None, 'row', 'col'), may hold values from 0 to 3
- tile_target: int32 [7, 4, 400], P(None, 'row', 'col'), may hold values from 0 to 7
Outputs:
- solution: float32 [4, 8, 8, 128, 256], P('row', 'col')
The draws below stay inside these ranges and needn't reach their ends.
All inputs are finite; a program needn't handle non-finite values.
Results may differ from the reference program's by a relative error of at most 0.017.
Values may be sent and summed in bfloat16 or wider, within the bound.
A program may use at most 128 MiB of HBM per device.

```python
import jax
import jax.numpy as jnp
from jax import lax

BLOCK = 128
SECTIONS = 8
TPD = 50
COLS = 256
N_ROW = 4
N_COL = 8


def plant(result, rng, least, high):
    place = [jax.random.randint(jax.random.fold_in(rng, axis), (), 0, length) for axis, length in enumerate(result.shape)]
    widest = result.shape.index(max(result.shape))
    beside = place[:widest] + [(place[widest] + 1) % result.shape[widest]] + place[widest + 1:]
    return result.at[tuple(place)].set(least).at[tuple(beside)].set(high)


def block_levels(key, extent, split, smallest, largest):
    loudness = 1.0
    for axis_at, parts in split:
        steps = jax.random.uniform(jax.random.fold_in(jax.random.fold_in(key, 6), axis_at), (parts,), jnp.float32, smallest / len(split), largest / len(split))
        loudness = loudness * jnp.repeat(jnp.exp(steps), extent[axis_at] // parts).reshape((-1,) + (1,) * (len(extent) - 1 - axis_at))
    return loudness


def scatter_about(own_key, extent, deviation, reach, pieces=(), kind=jnp.bfloat16):
    factor_of = block_levels(own_key, extent, pieces, -0.22, 0.18) if pieces else 1.0
    array = jax.random.normal(own_key, extent, jnp.float32) * deviation * factor_of
    return jnp.minimum(jnp.maximum(array, -reach), reach).astype(kind)


def setup_inputs(seed: int = 0) -> dict:
    seeds = jax.random.split(jax.random.key(seed), 6)
    right_side = scatter_about(seeds[0], (N_ROW, N_COL, SECTIONS, BLOCK, COLS), 1.0, 6.0, ((0, 4), (1, 8)))
    diag_inverse = scatter_about(seeds[1], (N_ROW, N_COL, SECTIONS, BLOCK, BLOCK), BLOCK ** -0.5, 0.5, ((0, 4), (1, 8)))
    panels = scatter_about(seeds[2], (SECTIONS - 1, N_ROW, N_COL * TPD, BLOCK, BLOCK), (2 * BLOCK * TPD) ** -0.5, 0.0546875, ((1, 4), (2, 8)))
    tile_source = plant(jax.random.randint(seeds[3], (SECTIONS - 1, N_ROW, N_COL * TPD), 0, N_ROW), jax.random.fold_in(seeds[3], 1), 0, N_ROW - 1).astype(jnp.int32)
    tile_target = plant(jax.random.randint(seeds[4], (SECTIONS - 1, N_ROW, N_COL * TPD), 0, N_COL), jax.random.fold_in(seeds[4], 1), 0, N_COL - 1).astype(jnp.int32)
    return dict(right_side=right_side, diag_inverse=diag_inverse, panels=panels, tile_source=tile_source, tile_target=tile_target)


def round_trip(values):
    low = lax.optimization_barrier(values.astype(jnp.bfloat16))
    return low.astype(jnp.float32)


def reference(right_side, diag_inverse, panels, tile_source, tile_target):
    solved = []
    incoming = jnp.zeros((N_ROW, N_COL, BLOCK, COLS), jnp.float32)
    for section in range(SECTIONS):
        current = right_side[:, :, section].astype(jnp.float32)
        if section > 0:
            current = current - incoming
        current = round_trip(current)
        block = jnp.einsum("ijab,ijbc->ijac", diag_inverse[:, :, section].astype(jnp.float32), current,
                           precision=lax.Precision.HIGHEST)
        solved.append(block)
        if section + 1 < SECTIONS:
            segment = round_trip(block)

            def row_update(items):
                panel_row, source_row, target_row = items
                column_of = (jnp.arange(N_COL * TPD, dtype=jnp.int32) // TPD).astype(jnp.int32)
                picked = segment[source_row, column_of]
                prods = jnp.einsum("qab,qbc->qac", panel_row.astype(jnp.float32), picked,
                                   precision=lax.Precision.HIGHEST)
                prods = prods.reshape(N_COL, TPD, BLOCK * COLS)
                targets = target_row.reshape(N_COL, TPD)
                onehot = (targets[:, None, :] == jnp.arange(N_COL, dtype=jnp.int32)[None, :, None]).astype(jnp.float32)
                shard_sums = jnp.einsum("jtq,jqe->jte", onehot, prods, precision=lax.Precision.HIGHEST)
                shard_sums = round_trip(shard_sums)
                return jnp.sum(shard_sums, axis=0).reshape(N_COL, BLOCK, COLS)

            incoming = lax.map(row_update, (panels[section], tile_source[section], tile_target[section]))
    return jnp.stack(solved, axis=2)
```

```python
import functools

import jax
import jax.numpy as jnp
from jax import lax
from jax.experimental import pallas as pl
from jax.experimental.pallas import tpu as pltpu
from jax.sharding import PartitionSpec as P

MESH = pl.DeviceIdType.MESH


def fold_kernel(rows, cols, source_ref, target_ref, panel_ref, out_ref, acc):
    level = pl.program_id(0)
    tiles, block = panel_ref.shape[2], panel_ref.shape[3]
    acc[...] = jnp.zeros_like(acc)

    def add(q, carry):
        target = target_ref[level, q]
        place = (target & 1) * (cols // 2) + (target >> 1)
        row = pl.multiple_of(place * block, block)
        column = pl.multiple_of(source_ref[level, q] * block, block)
        acc[pl.ds(row, block), pl.ds(column, block)] += panel_ref[0, 0, q].astype(jnp.float32)
        return carry

    lax.fori_loop(0, tiles, add, 0)
    out_ref[0] = acc[...].astype(out_ref.dtype)


def fold(panels, tile_source, tile_target, rows, cols):
    levels, _, tiles, block, _ = panels.shape
    return pl.pallas_call(
        functools.partial(fold_kernel, rows, cols),
        out_shape=jax.ShapeDtypeStruct((levels, cols * block, rows * block), jnp.bfloat16),
        grid_spec=pltpu.PrefetchScalarGridSpec(
            num_scalar_prefetch=2,
            grid=(levels,),
            in_specs=[pl.BlockSpec((1, 1, tiles, block, block), lambda s, *_: (s, 0, 0, 0, 0))],
            out_specs=pl.BlockSpec((1, cols * block, rows * block), lambda s, *_: (s, 0, 0)),
            scratch_shapes=[pltpu.VMEM((cols * block, rows * block), jnp.float32)],
        ),
        compiler_params=pltpu.CompilerParams(vmem_limit_bytes=56 * 1024 * 1024),
    )(tile_source[:, 0], tile_target[:, 0], panels)


def solve_kernel(rows, cols, window, right_ref, diag_ref, matrix_ref, out_ref,
                 matrix, gathered, pair_out, pair_in, own, shard_out, shard_in,
                 matrix_sem, gather_send, gather_recv, pair_send, pair_recv, shard_send, shard_recv):
    sections, block, width = right_ref.shape
    levels = sections - 1
    halves = gathered.shape[1]
    part = width // halves
    chips = cols // 2
    i, j = lax.axis_index("row"), lax.axis_index("col")
    z, core = j // 2, j % 2

    def row_peer(d):
        return (lax.rem(i + d, rows), j)

    def chip_peer(d):
        return (i, lax.rem(z + d, chips) * 2 + core)

    sibling = (i, z * 2 + 1 - core)

    def load(s):
        return pltpu.make_async_copy(matrix_ref.at[s], matrix.at[s % window], matrix_sem.at[s % window])

    for s in range(min(window, levels)):
        load(s).start()

    barrier = pltpu.get_barrier_semaphore()
    peers = [row_peer(d) for d in range(1, rows)] + [sibling] + [chip_peer(d) for d in range(1, chips)]
    for peer in peers:
        pl.semaphore_signal(barrier, inc=1, device_id=peer, device_id_type=MESH)
    pl.semaphore_wait(barrier, len(peers))

    def block_of(index):
        return pl.ds(pl.multiple_of(index * block, block), block)

    def gather_copy(p, h, d):
        here = gathered.at[p, h, block_of(i)]
        return pltpu.make_async_remote_copy(
            src_ref=here, dst_ref=here, send_sem=gather_send.at[p, h, d - 1], recv_sem=gather_recv.at[p, h, d - 1],
            device_id=row_peer(d), device_id_type=MESH)

    def pair_copy(p, h):
        return pltpu.make_async_remote_copy(
            src_ref=pair_out.at[p, h], dst_ref=pair_in.at[p, h], send_sem=pair_send.at[p, h],
            recv_sem=pair_recv.at[p, h], device_id=sibling, device_id_type=MESH)

    def shard_copy(p, h, d):
        return pltpu.make_async_remote_copy(
            src_ref=shard_out.at[p, h, block_of(lax.rem(z + d, chips))], dst_ref=shard_in.at[p, h, d - 1],
            send_sem=shard_send.at[p, h, d - 1], recv_sem=shard_recv.at[p, h, d - 1],
            device_id=chip_peer(d), device_id_type=MESH)

    def finish(s, h, incoming):
        columns = pl.ds(h * part, part)
        current = right_ref[s, :, columns].astype(jnp.float32)
        if incoming is not None:
            current = current - incoming
        solved = jnp.dot(diag_ref[s], current.astype(jnp.bfloat16), preferred_element_type=jnp.float32)
        out_ref[s, :, columns] = solved
        return solved.astype(jnp.bfloat16)

    def spread(s, h, segment):
        p = s % 2
        gathered[p, h, block_of(i), :] = segment
        for d in range(1, rows):
            gather_copy(p, h, d).start()

    def update(s, h):
        p = s % 2
        for d in range(1, rows):
            gather_copy(p, h, d).wait_recv()
        segment = gathered[p, h]
        tall = chips * block
        other = pl.ds(pl.multiple_of((1 - core) * tall, tall), tall)
        mine = pl.ds(pl.multiple_of(core * tall, tall), tall)
        pair_out[p, h] = jnp.dot(
            matrix[s % window, other, :], segment, preferred_element_type=jnp.float32).astype(jnp.bfloat16)
        pair_copy(p, h).start()
        own[h] = jnp.dot(matrix[s % window, mine, :], segment, preferred_element_type=jnp.float32)

    def combine(s, h):
        p = s % 2
        pair_copy(p, h).wait_recv()
        total = own[h] + pair_in[p, h].astype(jnp.float32)
        own[h] = total
        shard_out[p, h] = total.astype(jnp.bfloat16)
        for d in range(1, chips):
            shard_copy(p, h, d).start()

    def incoming_of(s, h):
        p = s % 2
        total = own[h, block_of(z), :]
        for d in range(1, chips):
            shard_copy(p, h, d).wait_recv()
        for d in range(1, chips):
            total = total + shard_in[p, h, d - 1].astype(jnp.float32)
        return total

    def drain(s, h):
        p = s % 2
        for d in range(1, rows):
            gather_copy(p, h, d).wait_send()
        pair_copy(p, h).wait_send()
        for d in range(1, chips):
            shard_copy(p, h, d).wait_send()

    def advance(s, last):
        load(s).wait()
        for h in range(halves):
            update(s, h)
        for h in range(halves):
            combine(s, h)
        if window < levels and not last:
            @pl.when(s + window < levels)
            def _():
                load(s + window).start()
        for h in range(halves):
            segment = finish(s + 1, h, incoming_of(s, h))
            if not last:
                spread(s + 1, h, segment)
        for h in range(halves):
            drain(s, h)

    for h in range(halves):
        spread(0, h, finish(0, h, None))

    def step(s, carry):
        advance(s, False)
        return carry

    lax.fori_loop(0, levels - 1, step, 0)
    advance(levels - 1, True)


def local(right_side, diag_inverse, panels, tile_source, tile_target):
    rows, cols = lax.axis_size("row"), lax.axis_size("col")
    sections, block, width = right_side.shape[2:]
    levels = sections - 1
    halves = 2 if width % 256 == 0 else 1
    part = width // halves
    chips = cols // 2
    matrix = fold(panels, tile_source, tile_target, rows, cols)
    window = levels if levels * matrix[0].size * 2 <= 24 * 1024 * 1024 else 2
    dma = pltpu.SemaphoreType.DMA
    vmem = pl.BlockSpec(memory_space=pltpu.VMEM)
    solved = pl.pallas_call(
        functools.partial(solve_kernel, rows, cols, window),
        out_shape=jax.ShapeDtypeStruct((sections, block, width), jnp.float32),
        in_specs=[vmem, vmem, pl.BlockSpec(memory_space=pl.ANY)],
        out_specs=vmem,
        scratch_shapes=[
            pltpu.VMEM((window, cols * block, rows * block), jnp.bfloat16),
            pltpu.VMEM((2, halves, rows * block, part), jnp.bfloat16),
            pltpu.VMEM((2, halves, chips * block, part), jnp.bfloat16),
            pltpu.VMEM((2, halves, chips * block, part), jnp.bfloat16),
            pltpu.VMEM((halves, chips * block, part), jnp.float32),
            pltpu.VMEM((2, halves, chips * block, part), jnp.bfloat16),
            pltpu.VMEM((2, halves, chips - 1, block, part), jnp.bfloat16),
            dma((window,)),
            dma((2, halves, rows - 1)),
            dma((2, halves, rows - 1)),
            dma((2, halves)),
            dma((2, halves)),
            dma((2, halves, chips - 1)),
            dma((2, halves, chips - 1)),
        ],
        compiler_params=pltpu.CompilerParams(
            collective_id=0, has_side_effects=True, vmem_limit_bytes=56 * 1024 * 1024),
    )(right_side[0, 0], diag_inverse[0, 0], matrix)
    return solved[None, None]


def solution(mesh):
    return jax.shard_map(
        local,
        mesh=mesh,
        in_specs=(
            P("row", "col", None, None, None),
            P("row", "col", None, None, None),
            P(None, "row", "col", None, None),
            P(None, "row", "col"),
            P(None, "row", "col"),
        ),
        out_specs=P("row", "col", None, None, None),
        check_vma=False,
    )
```

```python
import functools

import jax
import jax.numpy as jnp
from jax import lax
from jax.experimental import pallas as pl
from jax.experimental.pallas import tpu as pltpu
from jax.sharding import PartitionSpec as P

MESH = pl.DeviceIdType.MESH


def fold_links(tile_source, tile_target, rows, cols):
    tiles = tile_source.shape[1]
    place = (tile_target & 1) * (cols // 2) + (tile_target >> 1)
    key = place * rows + tile_source
    position = jnp.arange(tiles, dtype=jnp.int32)
    pairs = rows * cols
    want = jnp.concatenate([key, jnp.broadcast_to(jnp.arange(pairs, dtype=jnp.int32), (key.shape[0], pairs))], axis=1)
    limit = jnp.concatenate([position, jnp.full((pairs,), tiles, jnp.int32)])
    hit = (want[:, :, None] == key[:, None, :]) & (position[None, None, :] < limit[None, :, None])
    last = jnp.max(jnp.where(hit, position[None, None, :], -1), axis=2)
    return jnp.where(last < 0, tiles, last)


def solve_kernel(rows, cols, link_ref, right_ref, diag_ref, panel_ref, out_ref,
                 panels, runs, matrix, gathered, pair_out, pair_in, own, shard_out, shard_in,
                 panel_sem, gather_send, gather_recv, pair_send, pair_recv, shard_send, shard_recv):
    sections, block, width = right_ref.shape
    levels = sections - 1
    tiles = panels.shape[1]
    halves = gathered.shape[1]
    part = width // halves
    chips = cols // 2
    i, j = lax.axis_index("row"), lax.axis_index("col")
    z, core = j // 2, j % 2

    def row_peer(d):
        return (lax.rem(i + d, rows), j)

    def chip_peer(d):
        return (i, lax.rem(z + d, chips) * 2 + core)

    sibling = (i, z * 2 + 1 - core)

    def load(s):
        return pltpu.make_async_copy(panel_ref.at[s, 0], panels.at[s], panel_sem.at[s])

    for s in range(levels):
        load(s).start()

    barrier = pltpu.get_barrier_semaphore()
    peers = [row_peer(d) for d in range(1, rows)] + [sibling] + [chip_peer(d) for d in range(1, chips)]
    for peer in peers:
        pl.semaphore_signal(barrier, inc=1, device_id=peer, device_id_type=MESH)
    pl.semaphore_wait(barrier, len(peers))

    def block_of(index):
        return pl.ds(pl.multiple_of(index * block, block), block)

    def gather_copy(p, h, d):
        here = gathered.at[p, h, block_of(i)]
        return pltpu.make_async_remote_copy(
            src_ref=here, dst_ref=here, send_sem=gather_send.at[p, h, d - 1], recv_sem=gather_recv.at[p, h, d - 1],
            device_id=row_peer(d), device_id_type=MESH)

    def pair_copy(p, h):
        return pltpu.make_async_remote_copy(
            src_ref=pair_out.at[p, h], dst_ref=pair_in.at[p, h], send_sem=pair_send.at[p, h],
            recv_sem=pair_recv.at[p, h], device_id=sibling, device_id_type=MESH)

    def shard_copy(p, h, d):
        return pltpu.make_async_remote_copy(
            src_ref=shard_out.at[p, h, block_of(lax.rem(z + d, chips))], dst_ref=shard_in.at[p, h, d - 1],
            send_sem=shard_send.at[p, h, d - 1], recv_sem=shard_recv.at[p, h, d - 1],
            device_id=chip_peer(d), device_id_type=MESH)

    def finish(s, h, incoming):
        columns = pl.ds(h * part, part)
        current = right_ref[s, :, columns].astype(jnp.float32)
        if incoming is not None:
            current = current - incoming
        solved = jnp.dot(diag_ref[s], current.astype(jnp.bfloat16), preferred_element_type=jnp.float32)
        out_ref[s, :, columns] = solved
        return solved.astype(jnp.bfloat16)

    def spread(s, h, segment):
        p = s % 2
        gathered[p, h, block_of(i), :] = segment
        for d in range(1, rows):
            gather_copy(p, h, d).start()

    def update(s, h):
        p = s % 2
        for d in range(1, rows):
            gather_copy(p, h, d).wait_recv()
        segment = gathered[p, h]
        tall = chips * block
        other = pl.ds(pl.multiple_of((1 - core) * tall, tall), tall)
        mine = pl.ds(pl.multiple_of(core * tall, tall), tall)
        pair_out[p, h] = jnp.dot(
            matrix[s % 2, other, :], segment, preferred_element_type=jnp.float32).astype(jnp.bfloat16)
        pair_copy(p, h).start()
        own[h] = jnp.dot(matrix[s % 2, mine, :], segment, preferred_element_type=jnp.float32)

    def combine(s, h):
        p = s % 2
        pair_copy(p, h).wait_recv()
        total = own[h] + pair_in[p, h].astype(jnp.float32)
        own[h] = total
        shard_out[p, h] = total.astype(jnp.bfloat16)
        for d in range(1, chips):
            shard_copy(p, h, d).start()

    def incoming_of(s, h):
        p = s % 2
        total = own[h, block_of(z), :]
        for d in range(1, chips):
            shard_copy(p, h, d).wait_recv()
        for d in range(1, chips):
            total = total + shard_in[p, h, d - 1].astype(jnp.float32)
        return total

    def drain(s, h):
        p = s % 2
        for d in range(1, rows):
            gather_copy(p, h, d).wait_send()
        pair_copy(p, h).wait_send()
        for d in range(1, chips):
            shard_copy(p, h, d).wait_send()

    def fold(s):
        load(s).wait()

        def add(q, carry):
            runs[q] = panels[s, q].astype(jnp.float32) + runs[link_ref[s, q]]
            return carry

        def place(k, carry):
            matrix[s % 2, block_of(k // rows), block_of(k % rows)] = runs[link_ref[s, tiles + k]].astype(jnp.bfloat16)
            return carry

        lax.fori_loop(0, tiles, add, 0, unroll=2)
        lax.fori_loop(0, rows * cols, place, 0, unroll=4)

    def advance(s, last):
        for h in range(halves):
            update(s, h)
            combine(s, h)
        if not last:
            fold(s + 1)
        for h in range(halves):
            segment = finish(s + 1, h, incoming_of(s, h))
            if not last:
                spread(s + 1, h, segment)
        for h in range(halves):
            drain(s, h)

    for h in range(halves):
        spread(0, h, finish(0, h, None))
    runs[tiles] = jnp.zeros((block, block), jnp.float32)
    fold(0)

    def step(s, carry):
        advance(s, False)
        return carry

    lax.fori_loop(0, levels - 1, step, 0)
    advance(levels - 1, True)


def local(right_side, diag_inverse, panels, tile_source, tile_target):
    rows, cols = lax.axis_size("row"), lax.axis_size("col")
    sections, block, width = right_side.shape[2:]
    levels = sections - 1
    halves = 2 if width % 256 == 0 else 1
    part = width // halves
    chips = cols // 2
    tiles = panels.shape[2]
    links = fold_links(tile_source[:, 0], tile_target[:, 0], rows, cols)
    dma = pltpu.SemaphoreType.DMA
    vmem = pl.BlockSpec(memory_space=pltpu.VMEM)
    solved = pl.pallas_call(
        functools.partial(solve_kernel, rows, cols),
        out_shape=jax.ShapeDtypeStruct((sections, block, width), jnp.float32),
        in_specs=[pl.BlockSpec(memory_space=pltpu.SMEM), vmem, vmem, pl.BlockSpec(memory_space=pl.ANY)],
        out_specs=vmem,
        scratch_shapes=[
            pltpu.VMEM((levels, tiles, block, block), jnp.bfloat16),
            pltpu.VMEM((tiles + 1, block, block), jnp.float32),
            pltpu.VMEM((2, cols * block, rows * block), jnp.bfloat16),
            pltpu.VMEM((2, halves, rows * block, part), jnp.bfloat16),
            pltpu.VMEM((2, halves, chips * block, part), jnp.bfloat16),
            pltpu.VMEM((2, halves, chips * block, part), jnp.bfloat16),
            pltpu.VMEM((halves, chips * block, part), jnp.float32),
            pltpu.VMEM((2, halves, chips * block, part), jnp.bfloat16),
            pltpu.VMEM((2, halves, chips - 1, block, part), jnp.bfloat16),
            dma((levels,)),
            dma((2, halves, rows - 1)),
            dma((2, halves, rows - 1)),
            dma((2, halves)),
            dma((2, halves)),
            dma((2, halves, chips - 1)),
            dma((2, halves, chips - 1)),
        ],
        compiler_params=pltpu.CompilerParams(
            collective_id=0, has_side_effects=True, vmem_limit_bytes=56 * 1024 * 1024),
    )(links, right_side[0, 0], diag_inverse[0, 0], panels)
    return solved[None, None]


def solution(mesh):
    return jax.shard_map(
        local,
        mesh=mesh,
        in_specs=(
            P("row", "col", None, None, None),
            P("row", "col", None, None, None),
            P(None, "row", "col", None, None),
            P(None, "row", "col"),
            P(None, "row", "col"),
        ),
        out_specs=P("row", "col", None, None, None),
        check_vma=False,
    )
```
